32 devices in a mesh: section: 4 (over y, core), dp: 8 (over z, x).
Axes of the slice: x: 2, y: 2, z: 4, core: 2. Of those that a mesh axis runs over, the one named last changes fastest.
Arguments:
- tokens: bfloat16 [64, 6144], P('dp', 'section'), may hold values from -6 to 6
- expert_ids: int32 [64, 2], P('dp'), may hold values from 0 to 7, all different within a row; in each aligned block of 8 rows (0 to 7, 8 to 15, ...) at most 4 rows name the same one
- router: bfloat16 [6144, 8], replicated, may hold values from -0.078125 to 0.078125
- w_up: bfloat16 [8, 6144, 16384], P('dp', None, 'section'), may hold values from -0.078125 to 0.078125
- w_down: bfloat16 [8, 16384, 6144], P('dp', 'section'), may hold values from -0.0625 to 0.0625
- attn_queries: bfloat16 [8, 128, 6144], P('dp', None, 'section'), may hold values from -140 to 140
- attn_keys: bfloat16 [8, 128, 6144], P('dp', None, 'section'), may hold values from -8 to 8
- attn_values: bfloat16 [8, 128, 6144], P('dp', None, 'section'), may hold values from -6 to 6
Outputs:
- mixed: bfloat16 [64, 6144], P('dp', 'section')
- attended: bfloat16 [8, 128, 6144], P('dp', None, 'section')
The draws below stay inside these ranges and needn't reach their ends.
Inputs may be any that keep to these rules, and one draw needn't show every extreme that they name: `expert_ids`: each row names two different experts; among the 8 rows of one dp index (aligned blocks) no expert is named more than 4 times.
All inputs are finite; a program needn't handle non-finite values.
Results may differ from the reference program's by a relative error of at most 0.005.
Values may be sent and summed in bfloat16 or wider, within the bound.
A program may use at most 192 MiB of HBM per device.

```python
import math
import jax
import jax.numpy as jnp
import numpy as np
from jax import lax

D = 6144
FF = 16384
EXPERTS = 8
ATT_HEADS = 48
HEAD_DIM = 128
CAP = 4
TOK_DP = 8
SEQ = 128
RSPLIT = 1
TOKENS = 64
N_DP = 8


def attention_pair(key):
    base = jax.random.fold_in(key, 7)
    key_query, key_keys = jax.random.split(base, 2)
    shape = (N_DP, SEQ, ATT_HEADS * HEAD_DIM)
    key_array = jnp.clip(jax.random.normal(key_keys, shape, jnp.float32), -6.0, 6.0)
    query_array = jnp.clip(jax.random.normal(key_query, shape, jnp.float32), -6.0, 6.0)
    return (query_array, key_array)


def draw_attn_queries(key, part):
    query_array, key_array = attention_pair(key)
    return query_array.astype(jnp.bfloat16)


def draw_attn_keys(key, part):
    query_array, key_array = attention_pair(key)
    return key_array.astype(jnp.bfloat16)


def raised(result, rng, source, target, shards_of, factor):
    def block_of(position):
        return (jnp.arange(result.shape[position]) // (result.shape[position] // shards_of)).reshape((-1,) + (1,) * (result.ndim - 1 - position))

    near = jax.random.permutation(rng, shards_of)[block_of(target)]
    second = (block_of(target) + shards_of // 2) % shards_of
    return jnp.where((block_of(source) == near) | (block_of(source) == second), factor * result, result)


def levels(stream_key, extent, cuts, smallest, high):
    loudness, own = 1.0, jax.random.fold_in(stream_key, 6)
    for dim, blocks in cuts:
        draws = jnp.exp(jax.random.uniform(jax.random.fold_in(own, dim), (blocks,), jnp.float32, smallest / len(cuts), high / len(cuts)))
        loudness = loudness * jnp.repeat(draws, extent[dim] // blocks).reshape([-1 if axis == dim else 1 for axis in range(len(extent))])
    return loudness


def shared_out(key, own, number, rows, amount, top, limit, skew):
    sequence = jax.random.permutation(key, amount)
    packed, usual = shares(amount, rows * top, limit, skew, True), shares(amount, rows * top, limit, skew, False)
    places = jnp.arange(amount)

    def named(sizes, rotation):
        used = int((sizes > 0).sum())
        fixed = max(1, used // 4)
        passed = fixed + (places - fixed + rotation * (used - fixed)) % max(1, amount - fixed)
        return jnp.zeros((amount,), jnp.int32).at[sequence[jnp.where(places < fixed, places, passed)]].set(jnp.asarray(sizes, jnp.int32))

    sizes = jnp.where(number % 4 == 0, named(packed, number // 4), named(usual, number - number // 4 - 1))
    mixed = jax.random.permutation(jax.random.fold_in(own, 3), amount)
    giver, receiver = mixed[0:amount // 2 * 2:2], mixed[1:amount // 2 * 2:2]
    margin = jnp.minimum(sizes[giver] - 1, limit - sizes[receiver]) // 2
    margin = jnp.where((giver == sequence[0]) | (receiver == sequence[0]) | (sizes[receiver] == 0), 0, jnp.maximum(margin, 0))
    passed = jax.random.randint(jax.random.fold_in(own, 4), (amount // 2,), 0, 1 << 20) % (margin + 1)
    sizes = sizes.at[giver].add(-passed).at[receiver].add(passed)
    labels = jnp.searchsorted(jnp.cumsum(sizes), jnp.arange(rows * top), side="right").astype(jnp.int32)
    grid = labels.reshape(top, rows).T
    grid = grid[jax.random.permutation(jax.random.fold_in(own, 1), rows)]
    rotation = jax.random.randint(jax.random.fold_in(own, 2), (rows, 1), 0, top)
    return jnp.take_along_axis(grid, (jnp.arange(top)[None, :] + rotation) % top, axis=1)


def shares(count, total, limit, skew, full):
    loads = [(1 << 20) // math.isqrt(rank ** skew) + 1 for rank in range(1, count + 1)]
    largest = limit if full else min(limit, max(-(-total // count), total * loads[0] // sum(loads)))
    least = 1 if total - largest >= count - 1 else 0
    given, surplus = [largest] + [least] * (count - 1), total - largest - least * (count - 1)
    while surplus > 0:
        candidates = [i for i in range(1, count) if given[i] < largest] or [i for i in range(1, count) if given[i] < limit]
        mass, left = sum([loads[i] for i in candidates]), surplus
        for i in candidates:
            extra = min(limit - given[i], max(1, left * loads[i] // mass), surplus)
            given[i] = given[i] + extra
            surplus = surplus - extra
    return np.array(given)


def gaussian(stream_key, extent, deviation, most, cuts=(), held_as=jnp.bfloat16):
    entries = deviation * jax.random.normal(stream_key, extent, jnp.float32)
    if cuts:
        entries = entries * levels(stream_key, extent, cuts, -0.22, 0.18)
    return jnp.clip(entries, -most, most).astype(held_as)


def heavy_noise(stream_key, shape, spread, reach, pieces, heavy, held_as=jnp.bfloat16):
    result = spread * jax.random.normal(stream_key, shape, jnp.float32)
    if pieces:
        result = result * levels(stream_key, shape, pieces, -0.22, 0.18)
    return jnp.clip(raised(result, jax.random.fold_in(stream_key, 3), *heavy), -reach, reach).astype(held_as)


def setup_inputs(seed: int = 0) -> dict:
    key_of = jax.random.split(jax.random.key(seed), 9)
    tokens = gaussian(key_of[0], (TOKENS, D), 1.0, 6.0, ((0, 8), (1, 4)))
    expert_ids_keys = jax.random.split(jax.random.fold_in(key_of[1], 1), TOKENS // TOK_DP)
    expert_ids_turns = jax.random.permutation(jax.random.fold_in(key_of[1], 3), TOKENS // TOK_DP)
    expert_ids = jax.vmap(lambda own, number: shared_out(jax.random.fold_in(key_of[1], 2), own, number, TOK_DP, EXPERTS, 2, CAP, 2))(expert_ids_keys, expert_ids_turns).reshape((TOKENS, 2))
    router = gaussian(key_of[2], (D, EXPERTS), D ** -0.5, 0.078125)
    w_up = gaussian(key_of[3], (N_DP, D, FF // RSPLIT), D ** -0.5, 0.078125, ((0, 8), (2, 4)))
    w_down = heavy_noise(key_of[4], (N_DP, FF // RSPLIT, D), FF ** -0.5, 0.0625, ((0, 8), (1, 4)), (1, 2, 4, 2.0))
    attn_queries = draw_attn_queries(jax.random.fold_in(key_of[8], 71), 0)
    attn_keys = draw_attn_keys(jax.random.fold_in(key_of[8], 71), 0)
    attn_values = gaussian(key_of[7], (N_DP, SEQ, ATT_HEADS * HEAD_DIM), 1.0, 6.0, ((0, 8), (2, 4)))
    return dict(tokens=tokens, expert_ids=expert_ids, router=router, w_up=w_up, w_down=w_down, attn_queries=attn_queries, attn_keys=attn_keys, attn_values=attn_values)


def pair_weights(tokens, router, expert_ids):
    logits = jnp.dot(tokens, router, preferred_element_type=jnp.float32)
    experts = router.shape[1]
    onehot = (expert_ids[:, :, None] == jnp.arange(experts, dtype=jnp.int32)[None, None, :]).astype(jnp.float32)
    chosen = lax.optimization_barrier(jnp.sum(logits[:, None, :] * onehot, axis=2))
    first_prob = jax.nn.sigmoid(chosen[:, 0] - chosen[:, 1])
    return jnp.stack([first_prob, 1.0 - first_prob], axis=1)

def route_slots(expert_ids, block_count, per_block, experts):
    pair_ids = expert_ids.reshape(block_count, per_block * 2)
    onehot = (pair_ids[:, :, None] == jnp.arange(experts, dtype=jnp.int32)[None, None, :]).astype(jnp.int32)
    before = jnp.cumsum(onehot, axis=1) - onehot
    slot_rank = lax.optimization_barrier(jnp.sum(before * onehot, axis=2))
    return slot_rank.reshape(block_count * per_block, 2)

def attend_head(operands):
    head_queries, head_keys, head_values = operands
    length = head_queries.shape[0]
    scores = jnp.dot(head_queries, head_keys.T, preferred_element_type=jnp.float32) * (1.0 / math.sqrt(head_queries.shape[1]))
    positions = jnp.arange(length, dtype=jnp.int32)
    causal = positions[None, :] <= positions[:, None]
    scores = jnp.where(causal, scores, -jnp.inf)
    row_max = lax.optimization_barrier(jnp.max(scores, axis=1, keepdims=True))
    exp_scores = jnp.exp(scores - row_max)
    row_total = lax.optimization_barrier(jnp.sum(exp_scores, axis=1, keepdims=True))
    probs = (exp_scores / row_total).astype(jnp.bfloat16)
    return jnp.dot(probs, head_values, preferred_element_type=jnp.float32).astype(jnp.bfloat16)

def attention(attn_queries, attn_keys, attn_values):
    batch, length, width = attn_queries.shape
    heads = width // HEAD_DIM

    def split_heads(array):
        return jnp.transpose(array.reshape(batch, length, heads, HEAD_DIM), (0, 2, 1, 3)).reshape(batch * heads, length, HEAD_DIM)
    outputs = lax.map(attend_head, (split_heads(attn_queries), split_heads(attn_keys), split_heads(attn_values)))
    return jnp.transpose(outputs.reshape(batch, heads, length, HEAD_DIM), (0, 2, 1, 3)).reshape(batch, length, width)

def reference(tokens, expert_ids, router, w_up, w_down, attn_queries, attn_keys, attn_values):
    token_count, model_width = tokens.shape
    experts = router.shape[1]
    block_count = w_up.shape[0]
    split_count = block_count // experts
    per_block = token_count // block_count
    slot_count = block_count * CAP
    pair_prob = pair_weights(tokens, router, expert_ids)
    slot_rank = route_slots(expert_ids, block_count, per_block, experts)
    block_of = (jnp.arange(token_count, dtype=jnp.int32) // per_block)[:, None]
    slot_of = block_of * CAP + slot_rank
    slot_range = jnp.arange(slot_count, dtype=jnp.int32)
    token_rows = tokens.astype(jnp.float32)

    def one_expert(carried, expert):
        chosen_here = expert_ids == expert
        matched = (slot_of[:, :, None] == slot_range[None, None, :]) & chosen_here[:, :, None]
        selector = jnp.any(matched, axis=1).astype(jnp.float32)
        weighting = lax.optimization_barrier(jnp.sum(matched.astype(jnp.float32) * pair_prob[:, :, None], axis=1))
        rows = jnp.dot(selector.T, token_rows, precision=lax.Precision.HIGHEST).astype(jnp.bfloat16)
        first = (expert * split_count).astype(jnp.int32)
        up_part = lax.dynamic_slice_in_dim(w_up, first, split_count, 0)
        up_full = jnp.transpose(up_part, (1, 0, 2)).reshape(model_width, -1)
        down_full = lax.dynamic_slice_in_dim(w_down, first, split_count, 0).reshape(-1, model_width)
        activated = jax.nn.silu(jnp.dot(rows, up_full, preferred_element_type=jnp.float32)).astype(jnp.bfloat16)
        expert_out = jnp.dot(activated, down_full, preferred_element_type=jnp.float32)
        return (carried + jnp.dot(weighting, expert_out, precision=lax.Precision.HIGHEST), None)
    summed, _ = lax.scan(one_expert, jnp.zeros((token_count, model_width), jnp.float32), jnp.arange(experts, dtype=jnp.int32))
    attended = attention(attn_queries, attn_keys, attn_values)
    return (summed.astype(jnp.bfloat16), attended)
```

```python
import functools
import math

import jax
import jax.numpy as jnp
from jax import lax
from jax.experimental import pallas as pl
from jax.experimental.pallas import tpu as pltpu
from jax.sharding import PartitionSpec as P

HEAD_DIM = 128
LANES = 128
CAP = 4
MESH = pl.DeviceIdType.MESH


def aligned(index, size):
    return pl.ds(pl.multiple_of(index * size, size), size)


def kernel(
    dims,
    tokens_hbm,
    ids_hbm,
    router_hbm,
    up_hbm,
    down_hbm,
    q_hbm,
    k_hbm,
    v_hbm,
    mixed,
    attended,
    ring,
    tokens,
    outgoing,
    planes,
    x_rows,
    acc,
    hidden,
    stage,
    terms,
    returning,
    received,
    router,
    ids,
    logit_terms,
    coefficient,
    q,
    k,
    v,
    small_sem,
    up_sem,
    down_sem,
    send_sem,
    plane_sem,
    y_sem,
    pair_sem,
    logit_sem,
    term_sem,
    back_sem,
):
    n_sec, n_dp, cols, experts, fold, up_group, rows = dims
    per_block, width = tokens.shape
    ff = down_hbm.shape[1]
    slots, wide, part = per_block // fold, width // fold, cols // fold
    up_blocks, sec_blocks = ff // cols, width // cols
    groups, freed = up_blocks // up_group, up_group * width // rows
    down_units = ff // rows
    per_expert = n_dp // experts
    away = (n_sec - 1) * sec_blocks
    bf16, f32 = jnp.bfloat16, jnp.float32
    s, g = lax.axis_index("section"), lax.axis_index("dp")
    half = n_sec // 2
    y, core = s // 2, s % 2
    partner = {"section": y * 2 + 1 - core, "dp": g}

    def copy_in(index, source, target):
        return pltpu.make_async_copy(source, target, small_sem.at[index])

    copies = [
        copy_in(0, ids_hbm, ids),
        copy_in(1, tokens_hbm, tokens),
        copy_in(2, router_hbm.at[:, aligned(s, width)], router),
        copy_in(3, q_hbm.at[0], q),
        copy_in(4, k_hbm.at[0], k),
        copy_in(5, v_hbm.at[0], v),
    ]
    for copy in copies:
        copy.start()

    def section_of(j):
        return (y + half - j // 2) % half * 2 + (core + j) % 2

    def up_copy(j, n):
        unit = j * up_blocks + n
        return pltpu.make_async_copy(
            up_hbm.at[0, aligned(section_of(j), width), aligned(n, cols)],
            ring.at[aligned(unit, width)],
            up_sem.at[unit],
        )

    @pl.loop(0, n_sec * up_blocks)
    def _(unit):
        up_copy(unit // up_blocks, unit % up_blocks).start()

    barrier = pltpu.get_barrier_semaphore()

    def greet(place):
        pl.semaphore_signal(barrier, inc=1, device_id=place, device_id_type=MESH)

    @pl.loop(1, n_dp)
    def _(offset):
        greet({"section": s, "dp": (g + offset) % n_dp})

    @pl.loop(1, n_sec)
    def _(offset):
        greet({"section": (s + offset) % n_sec, "dp": g})

    def send(source, target, sems, place):
        pltpu.make_async_remote_copy(
            src_ref=source,
            dst_ref=target,
            send_sem=sems[0],
            recv_sem=sems[1],
            device_id=place,
            device_id_type=MESH,
        ).start()

    def await_bytes(like, sem):
        pltpu.make_async_copy(like, like, sem).wait()

    iota = functools.partial(lax.broadcasted_iota, jnp.int32)
    slot_bits, row_bits = slots.bit_length() - 1, per_block.bit_length() - 1

    def split_rows(index):
        within = index & (per_block - 1)
        return index >> row_bits, within >> slot_bits, within & (slots - 1)

    copies[0].wait()
    shape = (experts * per_block, per_block)
    expert, run, slot = split_rows(iota(shape, 0))
    named = (ids[0:1, :] == expert) | (ids[1:2, :] == expert)
    square = (per_block, per_block)
    earlier = (iota(square, 0) < iota(square, 1)).astype(f32).astype(bf16)
    rank = jnp.dot(named.astype(f32).astype(bf16), earlier, preferred_element_type=f32)
    picked = named & (rank == slot.astype(f32))
    copies[1].wait()
    packed = sum(
        jnp.dot(
            (picked & (run == h)).astype(f32).astype(bf16),
            tokens[:, h * wide : (h + 1) * wide],
            preferred_element_type=f32,
        )
        for h in range(fold)
    )
    for e in range(experts):
        outgoing[e] = packed[e * per_block : (e + 1) * per_block].astype(bf16)
    planes[s, g] = outgoing[g // per_expert]

    pl.semaphore_wait(barrier, n_dp + n_sec - 2)

    @pl.loop(1, n_dp)
    def _(offset):
        to = (g + offset) % n_dp
        send(
            outgoing.at[to // per_expert],
            planes.at[s, g],
            (send_sem.at[0], plane_sem),
            {"section": s, "dp": to},
        )

    copies[2].wait()
    partial = lax.dot_general(
        tokens[...], router[...], (((1,), (1,)), ((), ())), preferred_element_type=f32
    )
    logit_terms[s] = jnp.concatenate(
        [partial, jnp.zeros((per_block, LANES - experts), f32)], axis=1
    )

    @pl.loop(1, n_sec)
    def _(offset):
        send(
            logit_terms.at[s],
            logit_terms.at[s],
            (send_sem.at[2], logit_sem),
            {"section": (s + offset) % n_sec, "dp": g},
        )

    for copy in copies[3:]:
        copy.wait()
    length = q.shape[0]
    heads = width // HEAD_DIM
    together = math.gcd(heads, 4)
    causal = iota((length, length), 1) <= iota((length, length), 0)

    def attend(third):
        steps = heads // together
        pl.loop(steps * third // 3, steps * (third + 1) // 3)(attend_heads)

    def attend_heads(step):
        for lane in range(together):
            at = aligned(step * together + lane, HEAD_DIM)
            scores = lax.dot_general(
                q[:, at], k[:, at], (((1,), (1,)), ((), ())), preferred_element_type=f32
            ) * (1.0 / math.sqrt(HEAD_DIM))
            scores = jnp.where(causal, scores, -jnp.inf)
            exps = jnp.exp(scores - jnp.max(scores, axis=1, keepdims=True))
            probs = (exps / jnp.sum(exps, axis=1, keepdims=True)).astype(bf16)
            attended[0, :, at] = jnp.dot(
                probs, v[:, at], preferred_element_type=f32
            ).astype(bf16)

    attend(0)
    attend(1)

    def down_place(block):
        turn = block // sec_blocks
        to_y, to_core = (y + 1 + turn // 2) % half, (core + 1 + turn) % 2
        return to_y * 2 + to_core, block % sec_blocks

    def down_copy(unit):
        block, piece = unit // down_units, unit % down_units
        sec, col = down_place(block)
        return pltpu.make_async_copy(
            down_hbm.at[0, aligned(piece, rows), aligned(sec * sec_blocks + col, cols)],
            ring.at[aligned(unit, rows)],
            down_sem.at[block],
        )

    low = iota((per_block, 1), 0) < slots

    def exchange(first, second):
        turned = [pltpu.roll(value, slots, 0) for value in (first, second)]
        return jnp.where(low, first, turned[1]), jnp.where(low, turned[0], second)

    def assemble(j, sec):
        @pl.loop(0, n_dp // (2 * fold))
        def _(group):
            held = [
                planes[sec, group * (2 * fold) + b].astype(f32) for b in range(2 * fold)
            ]
            if fold == 2:
                pairs = [exchange(*held[:2]), exchange(*held[2:])]
                runs = [[pair[h] for pair in pairs] for h in range(2)]
            else:
                runs = [held]
            for h, run in enumerate(runs):
                x_rows[j, aligned(group, 2 * per_block), h * wide : (h + 1) * wide] = (
                    jnp.concatenate(run, axis=0).astype(bf16)
                )

    def phase(j, first, last):
        assemble(j, section_of(j))

        @pl.loop(0, groups)
        def _(group):
            for lane in range(up_group):
                up_copy(j, group * up_group + lane).wait()
            for lane in range(up_group):
                n = group * up_group + lane
                at = aligned(n, cols)
                value = jnp.dot(
                    x_rows[j],
                    ring[aligned(j * up_blocks + n, width), :],
                    preferred_element_type=f32,
                )
                if not first:
                    value += acc[:, at]
                if last:
                    hidden[:, at] = (value / (1.0 + jnp.exp(-value))).astype(bf16)
                else:
                    acc[:, at] = value

            @pl.loop(0, freed)
            def _(unit):
                down_copy((j * groups + group) * freed + unit).start()

    await_bytes(planes.at[s, pl.ds(0, n_dp - 1)], plane_sem)

    @pl.loop(1, half)
    def _(t):
        send(
            planes.at[s],
            planes.at[s],
            (send_sem.at[1], y_sem.at[t]),
            {"section": (y + t) % half * 2 + core, "dp": g},
        )

    send(planes.at[s], planes.at[s], (send_sem.at[1], pair_sem.at[0]), partner)
    phase(0, True, False)

    @pl.loop(1, n_sec - 1)
    def _(j):
        sec, t = section_of(j), j // 2

        @pl.when(j % 2 == 0)
        def _():
            await_bytes(planes.at[sec], y_sem.at[t])
            send(planes.at[sec], planes.at[sec], (send_sem.at[1], pair_sem.at[t]), partner)

        @pl.when(j % 2 == 1)
        def _():
            await_bytes(planes.at[sec], pair_sem.at[t])

        phase(j, False, False)

    await_bytes(planes.at[section_of(n_sec - 1)], pair_sem.at[half - 1])
    phase(n_sec - 1, False, True)
    attend(2)

    await_bytes(logit_terms.at[pl.ds(0, n_sec - 1)], logit_sem)
    logits = logit_terms[0]
    for sec in range(1, n_sec):
        logits += logit_terms[sec]
    diagonal = iota(square, 0) == iota(square, 1)

    def column(which):
        row = jnp.broadcast_to(ids[which : which + 1, :].astype(f32), diagonal.shape)
        return jnp.sum(jnp.where(diagonal, row, 0.0), axis=1, keepdims=True).astype(jnp.int32)

    first_id, second_id = column(0), column(1)
    lanes = iota((per_block, LANES), 1)

    def logit(which):
        return jnp.sum(jnp.where(lanes == which, logits, 0.0), axis=1, keepdims=True)

    first_prob = 1.0 / (1.0 + jnp.exp(logit(second_id) - logit(first_id)))
    source, run, slot = split_rows(iota((per_block, n_dp * per_block), 1))
    expert = source >> (per_expert.bit_length() - 1)
    is_first, is_second = first_id == expert, second_id == expert
    named = is_first | is_second
    before = (iota(square, 1) < iota(square, 0)).astype(f32).astype(bf16)
    rank = jnp.dot(before, named.astype(f32).astype(bf16), preferred_element_type=f32)
    weight = jnp.where(is_first, first_prob, 0.0) + jnp.where(is_second, 1.0 - first_prob, 0.0)
    weight = jnp.where(rank == slot.astype(f32), weight, 0.0)
    weights = jnp.concatenate(
        [jnp.where(run == h, weight, 0.0) for h in range(fold)], axis=0
    )
    coarse = weights.astype(bf16).astype(f32)
    coefficient[...] = jnp.concatenate([coarse, weights - coarse], axis=0).astype(bf16)

    def down_block(block):
        taken = ring.at[aligned(block, ff)]
        await_bytes(taken, down_sem.at[block])
        return jnp.dot(hidden[...], taken[...], preferred_element_type=f32)

    @pl.loop(0, away)
    def _(block):
        stage[block] = down_block(block).astype(bf16)
        sec, col = down_place(block)
        send(
            stage.at[block],
            terms.at[block // sec_blocks, :, aligned(col, cols)],
            (send_sem.at[3], term_sem),
            {"section": sec, "dp": g},
        )

    await_bytes(terms, term_sem)

    @pl.loop(0, sec_blocks)
    def _(block):
        summed = down_block(away + block)
        for term in range(n_sec - 1):
            summed += terms[term, :, aligned(block, cols)].astype(f32)
        for b in range(n_dp // fold):
            piece = summed[b * per_block : (b + 1) * per_block]
            if fold == 2:
                back = exchange(piece[:, :part], piece[:, part:])
            else:
                back = [piece]
            for i in range(fold):
                returning[block, b * fold + i] = back[i].astype(bf16)

        @pl.loop(1, n_dp)
        def _(offset):
            b = (g + offset) % n_dp
            send(
                returning.at[block, b],
                received.at[block, g],
                (send_sem.at[4], back_sem.at[block]),
                {"section": s, "dp": b},
            )

        received[block, g] = returning[block, g]

    @pl.loop(0, sec_blocks)
    def _(block):
        await_bytes(received.at[block, pl.ds(0, n_dp - 1)], back_sem.at[block])
        rows_back = jnp.concatenate(
            [received[block, b].astype(f32) for b in range(n_dp)], axis=0
        ).astype(bf16)
        both = jnp.dot(coefficient[...], rows_back, preferred_element_type=f32)
        tall = fold * per_block
        total = both[:tall] + both[tall:]
        for h in range(fold):
            at = pl.ds(pl.multiple_of(block * cols + h * part, part), part)
            mixed[:, at] = total[h * per_block : (h + 1) * per_block].astype(bf16)

    await_bytes(planes.at[0, pl.ds(0, n_dp - 1)], send_sem.at[0])
    await_bytes(planes.at[pl.ds(0, n_sec - 1)], send_sem.at[1])
    await_bytes(logit_terms.at[pl.ds(0, n_sec - 1)], send_sem.at[2])
    await_bytes(terms, send_sem.at[3])
    await_bytes(received.at[:, pl.ds(0, n_dp - 1)], send_sem.at[4])


def write_out(mixed, attended, mixed_hbm, attended_hbm, sems):
    copies = [
        pltpu.make_async_copy(mixed, mixed_hbm, sems.at[0]),
        pltpu.make_async_copy(attended, attended_hbm, sems.at[1]),
    ]
    for copy in copies:
        copy.start()
    for copy in copies:
        copy.wait()


def per_device(tokens, expert_ids, router, w_up, w_down, attn_queries, attn_keys, attn_values):
    n_sec, n_dp = lax.axis_size("section"), lax.axis_size("dp")
    per_block, width = tokens.shape
    model, experts = router.shape
    ff = w_up.shape[2]
    length = attn_queries.shape[1]
    cols = math.gcd(ff, width)
    fold = per_block // CAP if cols % (2 * LANES) == 0 else 1
    up_group = math.gcd(ff // cols, 4)
    rows = math.gcd(up_group * width, ff)
    slots, wide, part = per_block // fold, width // fold, cols // fold
    tall, down_blocks, sec_blocks = n_dp * slots, model // cols, width // cols
    bf16, f32 = jnp.bfloat16, jnp.float32
    any_spec = pl.BlockSpec(memory_space=pl.ANY)
    vmem_spec = pl.BlockSpec(memory_space=pltpu.VMEM)
    shapes = tokens.shape, attn_queries.shape
    held = pl.pallas_call(
        functools.partial(kernel, (n_sec, n_dp, cols, experts, fold, up_group, rows)),
        out_shape=tuple(pltpu.VMEM(shape, bf16) for shape in shapes),
        in_specs=[any_spec] * 8,
        out_specs=(vmem_spec, vmem_spec),
        scratch_shapes=[
            pltpu.VMEM((model * ff // cols, cols), bf16),
            pltpu.VMEM((per_block, width), bf16),
            pltpu.VMEM((experts, per_block, wide), bf16),
            pltpu.VMEM((n_sec, n_dp, per_block, wide), bf16),
            pltpu.VMEM((n_sec, tall, width), bf16),
            pltpu.VMEM((tall, ff), f32),
            pltpu.VMEM((tall, ff), bf16),
            pltpu.VMEM((down_blocks - sec_blocks, tall, cols), bf16),
            pltpu.VMEM((n_sec - 1, tall, width), bf16),
            pltpu.VMEM((sec_blocks, n_dp, per_block, part), bf16),
            pltpu.VMEM((sec_blocks, n_dp, per_block, part), bf16),
            pltpu.VMEM((experts, width), bf16),
            pltpu.VMEM((2, per_block), jnp.int32),
            pltpu.VMEM((n_sec, per_block, LANES), f32),
            pltpu.VMEM((2 * fold * per_block, n_dp * per_block), bf16),
            pltpu.VMEM((length, width), bf16),
            pltpu.VMEM((length, width), bf16),
            pltpu.VMEM((length, width), bf16),
            pltpu.SemaphoreType.DMA((6,)),
            pltpu.SemaphoreType.DMA((n_sec * ff // cols,)),
            pltpu.SemaphoreType.DMA((down_blocks,)),
            pltpu.SemaphoreType.DMA((5,)),
            pltpu.SemaphoreType.DMA,
            pltpu.SemaphoreType.DMA((n_sec // 2,)),
            pltpu.SemaphoreType.DMA((n_sec // 2,)),
            pltpu.SemaphoreType.DMA,
            pltpu.SemaphoreType.DMA,
            pltpu.SemaphoreType.DMA((sec_blocks,)),
        ],
        compiler_params=pltpu.CompilerParams(
            collective_id=0, has_side_effects=True, vmem_limit_bytes=62 * 2**20
        ),
    )(tokens, expert_ids.T, router.T, w_up, w_down, attn_queries, attn_keys, attn_values)
    return pl.pallas_call(
        write_out,
        out_shape=tuple(jax.ShapeDtypeStruct(shape, bf16) for shape in shapes),
        in_specs=[vmem_spec, vmem_spec],
        out_specs=(any_spec, any_spec),
        scratch_shapes=[pltpu.SemaphoreType.DMA((2,))],
    )(*(pltpu.with_memory_space_constraint(value, pltpu.VMEM) for value in held))


def solution(mesh):
    placed = (
        P("dp", "section"),
        P("dp", None),
        P(),
        P("dp", None, "section"),
        P("dp", "section", None),
        P("dp", None, "section"),
        P("dp", None, "section"),
        P("dp", None, "section"),
    )
    return jax.shard_map(
        per_device,
        mesh=mesh,
        in_specs=placed,
        out_specs=(P("dp", "section"), P("dp", None, "section")),
        check_vma=False,
    )
```

```python
import functools
import math

import jax
import jax.numpy as jnp
from jax import lax
from jax.experimental import pallas as pl
from jax.experimental.pallas import tpu as pltpu
from jax.sharding import PartitionSpec as P

HEAD_DIM = 128
LANES = 128
CAP = 4
MESH = pl.DeviceIdType.MESH


def aligned(index, size):
    return pl.ds(pl.multiple_of(index * size, size), size)


def kernel(
    dims,
    tokens_hbm,
    ids_hbm,
    router_hbm,
    up_hbm,
    down_hbm,
    q_hbm,
    k_hbm,
    v_hbm,
    mixed,
    attended,
    ring,
    tokens,
    outgoing,
    planes,
    x_rows,
    acc,
    hidden,
    stage,
    terms,
    returning,
    received,
    router,
    ids,
    logit_terms,
    coefficient,
    q,
    k,
    v,
    small_sem,
    up_sem,
    down_sem,
    own_sem,
    send_sem,
    plane_sem,
    y_sem,
    pair_sem,
    logit_sem,
    term_sem,
    back_sem,
):
    n_sec, n_dp, cols, experts, fold, tail, pieces = dims
    per_block, width = tokens.shape
    ff = down_hbm.shape[1]
    slots, wide, part = per_block // fold, width // fold, tail // fold
    ring_cols = ring.shape[1]
    up_runs, sec_blocks = ff // ring_cols, width // cols
    per_expert = n_dp // experts
    away, own = (n_sec - 1) * sec_blocks, width // tail
    bf16, f32 = jnp.bfloat16, jnp.float32
    s, g = lax.axis_index("section"), lax.axis_index("dp")
    half = n_sec // 2
    y, core = s // 2, s % 2
    partner = {"section": y * 2 + 1 - core, "dp": g}

    def copy_in(index, source, target):
        return pltpu.make_async_copy(source, target, small_sem.at[index])

    copies = [
        copy_in(0, ids_hbm, ids),
        copy_in(1, tokens_hbm, tokens),
        copy_in(2, router_hbm.at[:, aligned(s, width)], router),
        copy_in(3, q_hbm.at[0], q),
        copy_in(4, k_hbm.at[0], k),
        copy_in(5, v_hbm.at[0], v),
    ]
    for copy in copies:
        copy.start()

    def section_of(j):
        return (y + half - j // 2) % half * 2 + (core + j) % 2

    def up_copy(unit):
        return pltpu.make_async_copy(
            up_hbm.at[
                0, aligned(section_of(unit // up_runs), width), aligned(unit % up_runs, ring_cols)
            ],
            ring.at[aligned(unit, width)],
            up_sem.at[unit],
        )

    @pl.loop(0, n_sec * up_runs)
    def _(unit):
        up_copy(unit).start()

    barrier = pltpu.get_barrier_semaphore()

    def greet(place):
        pl.semaphore_signal(barrier, inc=1, device_id=place, device_id_type=MESH)

    @pl.loop(1, n_dp)
    def _(offset):
        greet({"section": s, "dp": (g + offset) % n_dp})

    @pl.loop(1, n_sec)
    def _(offset):
        greet({"section": (s + offset) % n_sec, "dp": g})

    def send(source, target, sems, place):
        pltpu.make_async_remote_copy(
            src_ref=source,
            dst_ref=target,
            send_sem=sems[0],
            recv_sem=sems[1],
            device_id=place,
            device_id_type=MESH,
        ).start()

    def await_bytes(like, sem):
        pltpu.make_async_copy(like, like, sem).wait()

    iota = functools.partial(lax.broadcasted_iota, jnp.int32)
    slot_bits, row_bits = slots.bit_length() - 1, per_block.bit_length() - 1

    def split_rows(index):
        within = index & (per_block - 1)
        return index >> row_bits, within >> slot_bits, within & (slots - 1)

    copies[0].wait()
    shape = (experts * per_block, per_block)
    expert, run, slot = split_rows(iota(shape, 0))
    named = (ids[0:1, :] == expert) | (ids[1:2, :] == expert)
    square = (per_block, per_block)
    earlier = (iota(square, 0) < iota(square, 1)).astype(f32).astype(bf16)
    rank = jnp.dot(named.astype(f32).astype(bf16), earlier, preferred_element_type=f32)
    picked = named & (rank == slot.astype(f32))
    copies[1].wait()
    packed = sum(
        jnp.dot(
            (picked & (run == h)).astype(f32).astype(bf16),
            tokens[:, h * wide : (h + 1) * wide],
            preferred_element_type=f32,
        )
        for h in range(fold)
    )
    for e in range(experts):
        outgoing[e] = packed[e * per_block : (e + 1) * per_block].astype(bf16)
    planes[s, g] = outgoing[g // per_expert]

    pl.semaphore_wait(barrier, n_dp + n_sec - 2)

    @pl.loop(1, n_dp)
    def _(offset):
        to = (g + offset) % n_dp
        send(
            outgoing.at[to // per_expert],
            planes.at[s, g],
            (send_sem.at[0], plane_sem),
            {"section": s, "dp": to},
        )

    copies[2].wait()
    partial = lax.dot_general(
        tokens[...], router[...], (((1,), (1,)), ((), ())), preferred_element_type=f32
    )
    logit_terms[s] = jnp.concatenate(
        [partial, jnp.zeros((per_block, LANES - experts), f32)], axis=1
    )

    @pl.loop(1, n_sec)
    def _(offset):
        send(
            logit_terms.at[s],
            logit_terms.at[s],
            (send_sem.at[2], logit_sem),
            {"section": (s + offset) % n_sec, "dp": g},
        )

    for copy in copies[3:]:
        copy.wait()
    length = q.shape[0]
    heads = width // HEAD_DIM
    together = math.gcd(heads, 4)
    causal = iota((length, length), 1) <= iota((length, length), 0)

    def attend(third):
        steps = heads // together
        pl.loop(steps * third // 3, steps * (third + 1) // 3)(attend_heads)

    def attend_heads(step):
        for lane in range(together):
            at = aligned(step * together + lane, HEAD_DIM)
            scores = lax.dot_general(
                q[:, at], k[:, at], (((1,), (1,)), ((), ())), preferred_element_type=f32
            ) * (1.0 / math.sqrt(HEAD_DIM))
            scores = jnp.where(causal, scores, -jnp.inf)
            exps = jnp.exp(scores - jnp.max(scores, axis=1, keepdims=True))
            probs = (exps / jnp.sum(exps, axis=1, keepdims=True)).astype(bf16)
            attended[0, :, at] = jnp.dot(
                probs, v[:, at], preferred_element_type=f32
            ).astype(bf16)

    attend(0)
    attend(1)

    def down_place(block):
        turn = block // sec_blocks
        to_y, to_core = (y + 1 + turn // 2) % half, (core + 1 + turn) % 2
        return to_y * 2 + to_core, block % sec_blocks

    def ring_at(index, size):
        return ring.at[aligned(index * size // ring_cols, ff), aligned(index % (ring_cols // size), size)]

    def down_copy(block):
        sec, col = down_place(block)
        return pltpu.make_async_copy(
            down_hbm.at[0, :, aligned(sec * sec_blocks + col, cols)],
            ring_at(block, cols),
            down_sem.at[block],
        )

    def own_at(index):
        return ring_at(away * cols // tail + index, tail)

    def own_copy(index):
        return pltpu.make_async_copy(
            down_hbm.at[0, :, aligned(s * own + index, tail)], own_at(index), own_sem.at[index]
        )

    def last_copy(piece):
        rows = aligned(piece, ff // pieces)
        return pltpu.make_async_copy(
            down_hbm.at[0, rows, aligned(s * own + own - 1, tail)],
            own_at(own - 1).at[rows],
            own_sem.at[own - 1 + piece],
        )

    low = iota((per_block, 1), 0) < slots

    def exchange(first, second):
        turned = [pltpu.roll(value, slots, 0) for value in (first, second)]
        return jnp.where(low, first, turned[1]), jnp.where(low, turned[0], second)

    def assemble(j, sec):
        @pl.loop(0, n_dp // (2 * fold))
        def _(group):
            held = [
                planes[sec, group * (2 * fold) + b].astype(f32) for b in range(2 * fold)
            ]
            if fold == 2:
                pairs = [exchange(*held[:2]), exchange(*held[2:])]
                runs = [[pair[h] for pair in pairs] for h in range(2)]
            else:
                runs = [held]
            for h, run in enumerate(runs):
                x_rows[j, aligned(group, 2 * per_block), h * wide : (h + 1) * wide] = (
                    jnp.concatenate(run, axis=0).astype(bf16)
                )

    def phase(j, first, last):
        assemble(j, section_of(j))

        for unit in range(j * up_runs, (j + 1) * up_runs):
            up_copy(unit).wait()
            for lane in range(ring_cols // cols):
                at = pl.ds(unit % up_runs * ring_cols + lane * cols, cols)
                value = jnp.dot(
                    x_rows[j],
                    ring[unit * width : (unit + 1) * width, lane * cols : (lane + 1) * cols],
                    preferred_element_type=f32,
                )
                if not first:
                    value += acc[:, at]
                if last:
                    hidden[:, at] = (value / (1.0 + jnp.exp(-value))).astype(bf16)
                else:
                    acc[:, at] = value
            start_down(unit)

    def start_down(unit):
        begin, end = (edge * width // ff * ring_cols for edge in (unit, unit + 1))
        bound = away * cols

        @pl.loop(min(begin, bound) // cols, min(end, bound) // cols)
        def _(block):
            down_copy(block).start()

        @pl.loop(max(begin - bound, 0) // tail, min(max(end - bound, 0) // tail, own - 1))
        def _(index):
            own_copy(index).start()

        if unit == n_sec * up_runs - 1:
            for piece in range(pieces):
                last_copy(piece).start()

    await_bytes(planes.at[s, pl.ds(0, n_dp - 1)], plane_sem)

    @pl.loop(1, half)
    def _(t):
        send(
            planes.at[s],
            planes.at[s],
            (send_sem.at[1], y_sem.at[t]),
            {"section": (y + t) % half * 2 + core, "dp": g},
        )

    send(planes.at[s], planes.at[s], (send_sem.at[1], pair_sem.at[0]), partner)
    phase(0, True, False)

    for j in range(1, n_sec):
        sec, t = section_of(j), j // 2
        if j % 2 == 0:
            await_bytes(planes.at[sec], y_sem.at[t])
            send(planes.at[sec], planes.at[sec], (send_sem.at[1], pair_sem.at[t]), partner)
        else:
            await_bytes(planes.at[sec], pair_sem.at[t])
        phase(j, False, j == n_sec - 1)

    attend(2)

    await_bytes(logit_terms.at[pl.ds(0, n_sec - 1)], logit_sem)
    logits = logit_terms[0]
    for sec in range(1, n_sec):
        logits += logit_terms[sec]
    diagonal = iota(square, 0) == iota(square, 1)

    def column(which):
        row = jnp.broadcast_to(ids[which : which + 1, :].astype(f32), diagonal.shape)
        return jnp.sum(jnp.where(diagonal, row, 0.0), axis=1, keepdims=True).astype(jnp.int32)

    first_id, second_id = column(0), column(1)
    lanes = iota((per_block, LANES), 1)

    def logit(which):
        return jnp.sum(jnp.where(lanes == which, logits, 0.0), axis=1, keepdims=True)

    first_prob = 1.0 / (1.0 + jnp.exp(logit(second_id) - logit(first_id)))
    source, run, slot = split_rows(iota((per_block, n_dp * per_block), 1))
    expert = source >> (per_expert.bit_length() - 1)
    is_first, is_second = first_id == expert, second_id == expert
    named = is_first | is_second
    before = (iota(square, 1) < iota(square, 0)).astype(f32).astype(bf16)
    rank = jnp.dot(before, named.astype(f32).astype(bf16), preferred_element_type=f32)
    weight = jnp.where(is_first, first_prob, 0.0) + jnp.where(is_second, 1.0 - first_prob, 0.0)
    weight = jnp.where(rank == slot.astype(f32), weight, 0.0)
    weights = jnp.concatenate(
        [jnp.where(run == h, weight, 0.0) for h in range(fold)], axis=0
    )
    coarse = weights.astype(bf16).astype(f32)
    coefficient[...] = jnp.concatenate([coarse, weights - coarse], axis=0).astype(bf16)

    def down_block(block):
        taken = ring_at(block, cols)
        await_bytes(taken, down_sem.at[block])
        return jnp.dot(hidden[...], taken[...], preferred_element_type=f32)

    @pl.loop(0, away)
    def _(block):
        stage[block] = down_block(block).astype(bf16)
        sec, col = down_place(block)
        send(
            stage.at[block],
            terms.at[block // sec_blocks, :, aligned(col, cols)],
            (send_sem.at[3], term_sem),
            {"section": sec, "dp": g},
        )

    await_bytes(terms, term_sem)

    def peers_terms(index):
        summed = terms[0, :, aligned(index, tail)].astype(f32)
        for term in range(1, n_sec - 1):
            summed += terms[term, :, aligned(index, tail)].astype(f32)
        return summed

    def give_back(index, summed):
        for b in range(n_dp // fold):
            piece = summed[b * per_block : (b + 1) * per_block]
            if fold == 2:
                back = exchange(piece[:, :part], piece[:, part:])
            else:
                back = [piece]
            for i in range(fold):
                returning[index, b * fold + i] = back[i].astype(bf16)

        @pl.loop(1, n_dp)
        def _(offset):
            b = (g + offset) % n_dp
            send(
                returning.at[index, b],
                received.at[index, g],
                (send_sem.at[4], back_sem.at[index]),
                {"section": s, "dp": b},
            )

        received[index, g] = returning[index, g]

    @pl.loop(0, own - 1)
    def _(index):
        taken = own_at(index)
        await_bytes(taken, own_sem.at[index])
        value = jnp.dot(hidden[...], taken[...], preferred_element_type=f32)
        give_back(index, value + peers_terms(index))

    summed = peers_terms(own - 1)
    for piece in range(pieces):
        rows = pl.ds(piece * (ff // pieces), ff // pieces)
        taken = own_at(own - 1).at[rows]
        await_bytes(taken, own_sem.at[own - 1 + piece])
        summed += jnp.dot(hidden[:, rows], taken[...], preferred_element_type=f32)
    give_back(own - 1, summed)

    @pl.loop(0, own)
    def _(index):
        await_bytes(received.at[index, pl.ds(0, n_dp - 1)], back_sem.at[index])
        rows_back = jnp.concatenate(
            [received[index, b].astype(f32) for b in range(n_dp)], axis=0
        ).astype(bf16)
        both = jnp.dot(coefficient[...], rows_back, preferred_element_type=f32)
        tall = fold * per_block
        total = both[:tall] + both[tall:]
        for h in range(fold):
            mixed[:, aligned(index * fold + h, part)] = total[
                h * per_block : (h + 1) * per_block
            ].astype(bf16)

    await_bytes(planes.at[0, pl.ds(0, n_dp - 1)], send_sem.at[0])
    await_bytes(planes.at[pl.ds(0, n_sec - 1)], send_sem.at[1])
    await_bytes(logit_terms.at[pl.ds(0, n_sec - 1)], send_sem.at[2])
    await_bytes(terms, send_sem.at[3])
    await_bytes(received.at[:, pl.ds(0, n_dp - 1)], send_sem.at[4])


def write_out(mixed, attended, mixed_hbm, attended_hbm, sems):
    copies = [
        pltpu.make_async_copy(mixed, mixed_hbm, sems.at[0]),
        pltpu.make_async_copy(attended, attended_hbm, sems.at[1]),
    ]
    for copy in copies:
        copy.start()
    for copy in copies:
        copy.wait()


def per_device(tokens, expert_ids, router, w_up, w_down, attn_queries, attn_keys, attn_values):
    n_sec, n_dp = lax.axis_size("section"), lax.axis_size("dp")
    per_block, width = tokens.shape
    model, experts = router.shape
    ff = w_up.shape[2]
    length = attn_queries.shape[1]
    cols = math.gcd(ff, width)
    ring_cols = math.gcd(ff, model)
    fold, tail = per_block // CAP if cols % (2 * LANES) == 0 else 1, cols
    pieces = math.gcd(ff // (2 * LANES), 4) if ff % (2 * LANES) == 0 else 1
    slots, wide, part, own = per_block // fold, width // fold, tail // fold, width // tail
    tall, sec_blocks = n_dp * slots, width // cols
    away = (n_sec - 1) * sec_blocks
    bf16, f32 = jnp.bfloat16, jnp.float32
    any_spec = pl.BlockSpec(memory_space=pl.ANY)
    vmem_spec = pl.BlockSpec(memory_space=pltpu.VMEM)
    shapes = tokens.shape, attn_queries.shape
    held = pl.pallas_call(
        functools.partial(kernel, (n_sec, n_dp, cols, experts, fold, tail, pieces)),
        out_shape=tuple(pltpu.VMEM(shape, bf16) for shape in shapes),
        in_specs=[any_spec] * 8,
        out_specs=(vmem_spec, vmem_spec),
        scratch_shapes=[
            pltpu.VMEM((model * ff // ring_cols, ring_cols), bf16),
            pltpu.VMEM((per_block, width), bf16),
            pltpu.VMEM((experts, per_block, wide), bf16),
            pltpu.VMEM((n_sec, n_dp, per_block, wide), bf16),
            pltpu.VMEM((n_sec, tall, width), bf16),
            pltpu.VMEM((tall, ff), f32),
            pltpu.VMEM((tall, ff), bf16),
            pltpu.VMEM((away, tall, cols), bf16),
            pltpu.VMEM((n_sec - 1, tall, width), bf16),
            pltpu.VMEM((own, n_dp, per_block, part), bf16),
            pltpu.VMEM((own, n_dp, per_block, part), bf16),
            pltpu.VMEM((experts, width), bf16),
            pltpu.VMEM((2, per_block), jnp.int32),
            pltpu.VMEM((n_sec, per_block, LANES), f32),
            pltpu.VMEM((2 * fold * per_block, n_dp * per_block), bf16),
            pltpu.VMEM((length, width), bf16),
            pltpu.VMEM((length, width), bf16),
            pltpu.VMEM((length, width), bf16),
            pltpu.SemaphoreType.DMA((6,)),
            pltpu.SemaphoreType.DMA((n_sec * ff // ring_cols,)),
            pltpu.SemaphoreType.DMA((away,)),
            pltpu.SemaphoreType.DMA((own - 1 + pieces,)),
            pltpu.SemaphoreType.DMA((5,)),
            pltpu.SemaphoreType.DMA,
            pltpu.SemaphoreType.DMA((n_sec // 2,)),
            pltpu.SemaphoreType.DMA((n_sec // 2,)),
            pltpu.SemaphoreType.DMA,
            pltpu.SemaphoreType.DMA,
            pltpu.SemaphoreType.DMA((own,)),
        ],
        compiler_params=pltpu.CompilerParams(
            collective_id=0, has_side_effects=True, vmem_limit_bytes=62 * 2**20
        ),
    )(tokens, expert_ids.T, router.T, w_up, w_down, attn_queries, attn_keys, attn_values)
    return pl.pallas_call(
        write_out,
        out_shape=tuple(jax.ShapeDtypeStruct(shape, bf16) for shape in shapes),
        in_specs=[vmem_spec, vmem_spec],
        out_specs=(any_spec, any_spec),
        scratch_shapes=[pltpu.SemaphoreType.DMA((2,))],
    )(*(pltpu.with_memory_space_constraint(value, pltpu.VMEM) for value in held))


def solution(mesh):
    placed = (
        P("dp", "section"),
        P("dp", None),
        P(),
        P("dp", None, "section"),
        P("dp", "section", None),
        P("dp", None, "section"),
        P("dp", None, "section"),
        P("dp", None, "section"),
    )
    return jax.shard_map(
        per_device,
        mesh=mesh,
        in_specs=placed,
        out_specs=(P("dp", "section"), P("dp", None, "section")),
        check_vma=False,
    )
```

```python
import functools
import math

import jax
import jax.numpy as jnp
from jax import lax
from jax.experimental import pallas as pl
from jax.experimental.pallas import tpu as pltpu
from jax.sharding import PartitionSpec as P

HEAD_DIM = 128
LANES = 128
CAP = 4
MESH = pl.DeviceIdType.MESH


def aligned(index, size):
    return pl.ds(pl.multiple_of(index * size, size), size)


def kernel(
    dims,
    tokens_hbm,
    ids_hbm,
    router_hbm,
    up_hbm,
    down_hbm,
    q_hbm,
    k_hbm,
    v_hbm,
    mixed,
    attended,
    ring,
    tokens,
    outgoing,
    planes,
    x_rows,
    acc,
    hidden,
    stage,
    terms,
    returning,
    received,
    router,
    ids,
    logit_terms,
    coefficient,
    q,
    k,
    v,
    small_sem,
    up_sem,
    down_sem,
    own_sem,
    send_sem,
    plane_sem,
    y_sem,
    pair_sem,
    logit_sem,
    term_sem,
    back_sem,
):
    n_sec, n_dp, cols, experts, fold, tail, pieces = dims
    per_block, width = tokens.shape
    ff = down_hbm.shape[1]
    slots, wide, part = per_block // fold, width // fold, tail // fold
    ring_cols = ring.shape[1]
    up_runs, sec_blocks = ff // ring_cols, width // cols
    per_expert = n_dp // experts
    away, own = (n_sec - 1) * sec_blocks, width // tail
    bf16, f32 = jnp.bfloat16, jnp.float32
    s, g = lax.axis_index("section"), lax.axis_index("dp")
    half = n_sec // 2
    y, core = s // 2, s % 2
    partner = {"section": y * 2 + 1 - core, "dp": g}

    def copy_in(index, source, target):
        return pltpu.make_async_copy(source, target, small_sem.at[index])

    copies = [
        copy_in(0, ids_hbm, ids),
        copy_in(1, tokens_hbm, tokens),
        copy_in(2, router_hbm.at[:, aligned(s, width)], router),
        copy_in(3, q_hbm.at[0], q),
        copy_in(4, k_hbm.at[0], k),
        copy_in(5, v_hbm.at[0], v),
    ]
    for copy in copies:
        copy.start()

    def section_of(j):
        return (y + half - j // 2) % half * 2 + (core + j) % 2

    def up_copy(unit):
        return pltpu.make_async_copy(
            up_hbm.at[
                0, aligned(section_of(unit // up_runs), width), aligned(unit % up_runs, ring_cols)
            ],
            ring.at[aligned(unit, width)],
            up_sem.at[unit],
        )

    @pl.loop(0, n_sec * up_runs)
    def _(unit):
        up_copy(unit).start()

    barrier = pltpu.get_barrier_semaphore()

    def greet(place):
        pl.semaphore_signal(barrier, inc=1, device_id=place, device_id_type=MESH)

    @pl.loop(1, n_dp)
    def _(offset):
        greet({"section": s, "dp": (g + offset) % n_dp})

    @pl.loop(1, n_sec)
    def _(offset):
        greet({"section": (s + offset) % n_sec, "dp": g})

    def send(source, target, sems, place):
        pltpu.make_async_remote_copy(
            src_ref=source,
            dst_ref=target,
            send_sem=sems[0],
            recv_sem=sems[1],
            device_id=place,
            device_id_type=MESH,
        ).start()

    def await_bytes(like, sem):
        pltpu.make_async_copy(like, like, sem).wait()

    iota = functools.partial(lax.broadcasted_iota, jnp.int32)
    slot_bits, row_bits = slots.bit_length() - 1, per_block.bit_length() - 1

    def split_rows(index):
        within = index & (per_block - 1)
        return index >> row_bits, within >> slot_bits, within & (slots - 1)

    copies[0].wait()
    shape = (experts * per_block, per_block)
    expert, run, slot = split_rows(iota(shape, 0))
    named = (ids[0:1, :] == expert) | (ids[1:2, :] == expert)
    square = (per_block, per_block)
    earlier = (iota(square, 0) < iota(square, 1)).astype(f32).astype(bf16)
    rank = jnp.dot(named.astype(f32).astype(bf16), earlier, preferred_element_type=f32)
    picked = named & (rank == slot.astype(f32))
    copies[1].wait()
    packed = sum(
        jnp.dot(
            (picked & (run == h)).astype(f32).astype(bf16),
            tokens[:, h * wide : (h + 1) * wide],
            preferred_element_type=f32,
        )
        for h in range(fold)
    )
    for e in range(experts):
        outgoing[e] = packed[e * per_block : (e + 1) * per_block].astype(bf16)
    planes[s, g] = outgoing[g // per_expert]

    pl.semaphore_wait(barrier, n_dp + n_sec - 2)

    @pl.loop(1, n_dp)
    def _(offset):
        to = (g + offset) % n_dp
        send(
            outgoing.at[to // per_expert],
            planes.at[s, g],
            (send_sem.at[0], plane_sem),
            {"section": s, "dp": to},
        )

    copies[2].wait()
    partial = lax.dot_general(
        tokens[...], router[...], (((1,), (1,)), ((), ())), preferred_element_type=f32
    )
    logit_terms[s] = jnp.concatenate(
        [partial, jnp.zeros((per_block, LANES - experts), f32)], axis=1
    )

    @pl.loop(1, n_sec)
    def _(offset):
        send(
            logit_terms.at[s],
            logit_terms.at[s],
            (send_sem.at[2], logit_sem),
            {"section": (s + offset) % n_sec, "dp": g},
        )

    for copy in copies[3:]:
        copy.wait()
    length = q.shape[0]
    heads = width // HEAD_DIM
    together = math.gcd(heads, 4)
    causal = iota((length, length), 1) <= iota((length, length), 0)

    def attend(third):
        steps = heads // together
        pl.loop(steps * third // 3, steps * (third + 1) // 3)(attend_heads)

    def attend_heads(step):
        for lane in range(together):
            at = aligned(step * together + lane, HEAD_DIM)
            scores = lax.dot_general(
                q[:, at], k[:, at], (((1,), (1,)), ((), ())), preferred_element_type=f32
            ) * (1.0 / math.sqrt(HEAD_DIM))
            scores = jnp.where(causal, scores, -jnp.inf)
            exps = jnp.exp(scores - jnp.max(scores, axis=1, keepdims=True))
            probs = (exps / jnp.sum(exps, axis=1, keepdims=True)).astype(bf16)
            attended[0, :, at] = jnp.dot(
                probs, v[:, at], preferred_element_type=f32
            ).astype(bf16)

    attend(0)
    attend(1)

    def down_place(block):
        turn = block // sec_blocks
        to_y, to_core = (y + 1 + turn // 2) % half, (core + 1 + turn) % 2
        return to_y * 2 + to_core, block % sec_blocks

    def ring_at(index, size):
        return ring.at[aligned(index * size // ring_cols, ff), aligned(index % (ring_cols // size), size)]

    def down_copy(block):
        sec, col = down_place(block)
        return pltpu.make_async_copy(
            down_hbm.at[0, :, aligned(sec * sec_blocks + col, cols)],
            ring_at(block, cols),
            down_sem.at[block],
        )

    def own_at(index):
        return ring_at(away * cols // tail + index, tail)

    def own_copy(index, piece):
        rows = aligned(piece, ff // pieces)
        return pltpu.make_async_copy(
            down_hbm.at[0, rows, aligned(s * own + index, tail)],
            own_at(index).at[rows],
            own_sem.at[index * pieces + piece],
        )

    low = iota((per_block, 1), 0) < slots

    def exchange(first, second):
        turned = [pltpu.roll(value, slots, 0) for value in (first, second)]
        return jnp.where(low, first, turned[1]), jnp.where(low, turned[0], second)

    def assemble(j, sec):
        @pl.loop(0, n_dp // (2 * fold))
        def _(group):
            held = [
                planes[sec, group * (2 * fold) + b].astype(f32) for b in range(2 * fold)
            ]
            if fold == 2:
                pairs = [exchange(*held[:2]), exchange(*held[2:])]
                runs = [[pair[h] for pair in pairs] for h in range(2)]
            else:
                runs = [held]
            for h, run in enumerate(runs):
                x_rows[j, aligned(group, 2 * per_block), h * wide : (h + 1) * wide] = (
                    jnp.concatenate(run, axis=0).astype(bf16)
                )

    def phase(j, first, last):
        assemble(j, section_of(j))

        for unit in range(j * up_runs, (j + 1) * up_runs):
            up_copy(unit).wait()
            for lane in range(ring_cols // cols):
                at = pl.ds(unit % up_runs * ring_cols + lane * cols, cols)
                value = jnp.dot(
                    x_rows[j],
                    ring[unit * width : (unit + 1) * width, lane * cols : (lane + 1) * cols],
                    preferred_element_type=f32,
                )
                if not first:
                    value += acc[:, at]
                if last:
                    hidden[:, at] = (value / (1.0 + jnp.exp(-value))).astype(bf16)
                else:
                    acc[:, at] = value
            start_down(unit)

    def start_down(unit):
        begin, end = (edge * width // ff * ring_cols for edge in (unit, unit + 1))
        bound = away * cols

        @pl.loop(min(begin, bound) // cols, min(end, bound) // cols)
        def _(block):
            down_copy(block).start()

        @pl.loop(max(begin - bound, 0) // tail, max(end - bound, 0) // tail)
        def _(index):
            for piece in range(pieces):
                own_copy(index, piece).start()

    await_bytes(planes.at[s, pl.ds(0, n_dp - 1)], plane_sem)

    @pl.loop(1, half)
    def _(t):
        send(
            planes.at[s],
            planes.at[s],
            (send_sem.at[1], y_sem.at[t]),
            {"section": (y + t) % half * 2 + core, "dp": g},
        )

    send(planes.at[s], planes.at[s], (send_sem.at[1], pair_sem.at[0]), partner)
    phase(0, True, False)

    for j in range(1, n_sec):
        sec, t = section_of(j), j // 2
        if j % 2 == 0:
            await_bytes(planes.at[sec], y_sem.at[t])
            send(planes.at[sec], planes.at[sec], (send_sem.at[1], pair_sem.at[t]), partner)
        else:
            await_bytes(planes.at[sec], pair_sem.at[t])
        phase(j, False, j == n_sec - 1)

    attend(2)

    await_bytes(logit_terms.at[pl.ds(0, n_sec - 1)], logit_sem)
    logits = logit_terms[0]
    for sec in range(1, n_sec):
        logits += logit_terms[sec]
    diagonal = iota(square, 0) == iota(square, 1)

    def column(which):
        row = jnp.broadcast_to(ids[which : which + 1, :].astype(f32), diagonal.shape)
        return jnp.sum(jnp.where(diagonal, row, 0.0), axis=1, keepdims=True).astype(jnp.int32)

    first_id, second_id = column(0), column(1)
    lanes = iota((per_block, LANES), 1)

    def logit(which):
        return jnp.sum(jnp.where(lanes == which, logits, 0.0), axis=1, keepdims=True)

    first_prob = 1.0 / (1.0 + jnp.exp(logit(second_id) - logit(first_id)))
    source, run, slot = split_rows(iota((per_block, n_dp * per_block), 1))
    expert = source >> (per_expert.bit_length() - 1)
    is_first, is_second = first_id == expert, second_id == expert
    named = is_first | is_second
    before = (iota(square, 1) < iota(square, 0)).astype(f32).astype(bf16)
    rank = jnp.dot(before, named.astype(f32).astype(bf16), preferred_element_type=f32)
    weight = jnp.where(is_first, first_prob, 0.0) + jnp.where(is_second, 1.0 - first_prob, 0.0)
    weight = jnp.where(rank == slot.astype(f32), weight, 0.0)
    weights = jnp.concatenate(
        [jnp.where(run == h, weight, 0.0) for h in range(fold)], axis=0
    )
    coarse = weights.astype(bf16).astype(f32)
    coefficient[...] = jnp.concatenate([coarse, weights - coarse], axis=0).astype(bf16)

    def down_block(block):
        taken = ring_at(block, cols)
        await_bytes(taken, down_sem.at[block])
        return jnp.dot(hidden[...], taken[...], preferred_element_type=f32)

    @pl.loop(0, away)
    def _(block):
        stage[block] = down_block(block).astype(bf16)
        sec, col = down_place(block)
        send(
            stage.at[block],
            terms.at[block // sec_blocks, :, aligned(col, cols)],
            (send_sem.at[3], term_sem),
            {"section": sec, "dp": g},
        )

    await_bytes(terms, term_sem)

    def peers_terms(index):
        summed = terms[0, :, aligned(index, tail)].astype(f32)
        for term in range(1, n_sec - 1):
            summed += terms[term, :, aligned(index, tail)].astype(f32)
        return summed

    def give_back(index, summed):
        for b in range(n_dp // fold):
            piece = summed[b * per_block : (b + 1) * per_block]
            if fold == 2:
                back = exchange(piece[:, :part], piece[:, part:])
            else:
                back = [piece]
            for i in range(fold):
                returning[index, b * fold + i] = back[i].astype(bf16)

        @pl.loop(1, n_dp)
        def _(offset):
            b = (g + offset) % n_dp
            send(
                returning.at[index, b],
                received.at[index, g],
                (send_sem.at[4], back_sem.at[index]),
                {"section": s, "dp": b},
            )

        received[index, g] = returning[index, g]

    @pl.loop(0, own)
    def _(index):
        summed = peers_terms(index)
        for piece in range(pieces):
            rows = pl.ds(piece * (ff // pieces), ff // pieces)
            taken = own_at(index).at[rows]
            await_bytes(taken, own_sem.at[index * pieces + piece])
            summed += jnp.dot(hidden[:, rows], taken[...], preferred_element_type=f32)
        give_back(index, summed)

    @pl.loop(0, own)
    def _(index):
        await_bytes(received.at[index, pl.ds(0, n_dp - 1)], back_sem.at[index])
        rows_back = jnp.concatenate(
            [received[index, b].astype(f32) for b in range(n_dp)], axis=0
        ).astype(bf16)
        both = jnp.dot(coefficient[...], rows_back, preferred_element_type=f32)
        tall = fold * per_block
        total = both[:tall] + both[tall:]
        for h in range(fold):
            mixed[:, aligned(index * fold + h, part)] = total[
                h * per_block : (h + 1) * per_block
            ].astype(bf16)

    await_bytes(planes.at[0, pl.ds(0, n_dp - 1)], send_sem.at[0])
    await_bytes(planes.at[pl.ds(0, n_sec - 1)], send_sem.at[1])
    await_bytes(logit_terms.at[pl.ds(0, n_sec - 1)], send_sem.at[2])
    await_bytes(terms, send_sem.at[3])
    await_bytes(received.at[:, pl.ds(0, n_dp - 1)], send_sem.at[4])


def write_out(mixed, attended, mixed_hbm, attended_hbm, sems):
    copies = [
        pltpu.make_async_copy(mixed, mixed_hbm, sems.at[0]),
        pltpu.make_async_copy(attended, attended_hbm, sems.at[1]),
    ]
    for copy in copies:
        copy.start()
    for copy in copies:
        copy.wait()


def per_device(tokens, expert_ids, router, w_up, w_down, attn_queries, attn_keys, attn_values):
    n_sec, n_dp = lax.axis_size("section"), lax.axis_size("dp")
    per_block, width = tokens.shape
    model, experts = router.shape
    ff = w_up.shape[2]
    length = attn_queries.shape[1]
    cols = math.gcd(ff, width)
    ring_cols = math.gcd(ff, model)
    fold, tail = per_block // CAP if cols % (2 * LANES) == 0 else 1, cols
    pieces = math.gcd(ff // (2 * LANES), 2) if ff % (2 * LANES) == 0 else 1
    slots, wide, part, own = per_block // fold, width // fold, tail // fold, width // tail
    tall, sec_blocks = n_dp * slots, width // cols
    away = (n_sec - 1) * sec_blocks
    bf16, f32 = jnp.bfloat16, jnp.float32
    any_spec = pl.BlockSpec(memory_space=pl.ANY)
    vmem_spec = pl.BlockSpec(memory_space=pltpu.VMEM)
    shapes = tokens.shape, attn_queries.shape
    held = pl.pallas_call(
        functools.partial(kernel, (n_sec, n_dp, cols, experts, fold, tail, pieces)),
        out_shape=tuple(pltpu.VMEM(shape, bf16) for shape in shapes),
        in_specs=[any_spec] * 8,
        out_specs=(vmem_spec, vmem_spec),
        scratch_shapes=[
            pltpu.VMEM((model * ff // ring_cols, ring_cols), bf16),
            pltpu.VMEM((per_block, width), bf16),
            pltpu.VMEM((experts, per_block, wide), bf16),
            pltpu.VMEM((n_sec, n_dp, per_block, wide), bf16),
            pltpu.VMEM((n_sec, tall, width), bf16),
            pltpu.VMEM((tall, ff), f32),
            pltpu.VMEM((tall, ff), bf16),
            pltpu.VMEM((away, tall, cols), bf16),
            pltpu.VMEM((n_sec - 1, tall, width), bf16),
            pltpu.VMEM((own, n_dp, per_block, part), bf16),
            pltpu.VMEM((own, n_dp, per_block, part), bf16),
            pltpu.VMEM((experts, width), bf16),
            pltpu.VMEM((2, per_block), jnp.int32),
            pltpu.VMEM((n_sec, per_block, LANES), f32),
            pltpu.VMEM((2 * fold * per_block, n_dp * per_block), bf16),
            pltpu.VMEM((length, width), bf16),
            pltpu.VMEM((length, width), bf16),
            pltpu.VMEM((length, width), bf16),
            pltpu.SemaphoreType.DMA((6,)),
            pltpu.SemaphoreType.DMA((n_sec * ff // ring_cols,)),
            pltpu.SemaphoreType.DMA((away,)),
            pltpu.SemaphoreType.DMA((own * pieces,)),
            pltpu.SemaphoreType.DMA((5,)),
            pltpu.SemaphoreType.DMA,
            pltpu.SemaphoreType.DMA((n_sec // 2,)),
            pltpu.SemaphoreType.DMA((n_sec // 2,)),
            pltpu.SemaphoreType.DMA,
            pltpu.SemaphoreType.DMA,
            pltpu.SemaphoreType.DMA((own,)),
        ],
        compiler_params=pltpu.CompilerParams(
            collective_id=0, has_side_effects=True, vmem_limit_bytes=62 * 2**20
        ),
    )(tokens, expert_ids.T, router.T, w_up, w_down, attn_queries, attn_keys, attn_values)
    return pl.pallas_call(
        write_out,
        out_shape=tuple(jax.ShapeDtypeStruct(shape, bf16) for shape in shapes),
        in_specs=[vmem_spec, vmem_spec],
        out_specs=(any_spec, any_spec),
        scratch_shapes=[pltpu.SemaphoreType.DMA((2,))],
    )(*(pltpu.with_memory_space_constraint(value, pltpu.VMEM) for value in held))


def solution(mesh):
    placed = (
        P("dp", "section"),
        P("dp", None),
        P(),
        P("dp", None, "section"),
        P("dp", "section", None),
        P("dp", None, "section"),
        P("dp", None, "section"),
        P("dp", None, "section"),
    )
    return jax.shard_map(
        per_device,
        mesh=mesh,
        in_specs=placed,
        out_specs=(P("dp", "section"), P("dp", None, "section")),
        check_vma=False,
    )
```
